64 devices in a mesh: rep: 8 (over x, y, core), dp: 8 (over z).
Axes of the slice: x: 2, y: 2, z: 8, core: 2. Of those that a mesh axis runs over, the one named last changes fastest.
The devices are a block of a 4x4x8 slice.
Arguments:
- x: bfloat16 [64, 2048, 640], P(('rep', 'dp')), parts along dimension 0
- dy: bfloat16 [64, 2048, 640], P(('rep', 'dp')), parts along dimension 0
- w_gate: bfloat16 [2, 640, 2176], replicated
- w_up: bfloat16 [2, 640, 2176], replicated
- w_down: bfloat16 [2, 2176, 640], replicated
- m_w_gate: float32 [2, 640, 2176], replicated
- m_w_up: float32 [2, 640, 2176], replicated
- m_w_down: float32 [2, 2176, 640], replicated
- v_w_gate: float32 [2, 640, 2176], replicated
- v_w_up: float32 [2, 640, 2176], replicated
- v_w_down: float32 [2, 2176, 640], replicated
Outputs:
- output 1: bfloat16 [16, 640, 2176], P('rep'), parts along dimension 0
- output 2: bfloat16 [16, 640, 2176], P('rep'), parts along dimension 0
- output 3: bfloat16 [16, 2176, 640], P('rep'), parts along dimension 0
- output 4: float32 [16, 640, 2176], P('rep'), parts along dimension 0
- output 5: float32 [16, 640, 2176], P('rep'), parts along dimension 0
- output 6: float32 [16, 2176, 640], P('rep'), parts along dimension 0
- output 7: float32 [16, 640, 2176], P('rep'), parts along dimension 0
- output 8: float32 [16, 640, 2176], P('rep'), parts along dimension 0
- output 9: float32 [16, 2176, 640], P('rep'), parts along dimension 0
There are 8 independent parts. The reference program is written for one: setup_inputs(seed, part) draws one part's arguments, and reference() takes and returns one part's arrays. A program takes and returns all parts, laid end to end along the dimension named above; an argument that names none is the same for every part.
All inputs are finite; a program needn't handle non-finite values.
Results may differ from the reference program's by a relative error of at most 0.022.
Values are sent between devices in bfloat16 or wider.
A program may use at most 768 MiB of HBM per device.

```python
import jax
import jax.numpy as jnp
from jax import lax

SEQUENCES = 8
TOKENS = 2048
D = 640
FF = 2176
LAYERS = 2
NAMES = ("w_gate", "w_up", "w_down")
SHAPES = {"w_gate": (LAYERS, D, FF), "w_up": (LAYERS, D, FF), "w_down": (LAYERS, FF, D)}


def bump(key, n, height):
    away = (jnp.arange(n, dtype=jnp.int32) - jax.random.randint(key, (), 0, n, jnp.int32)) % n
    return jnp.where(away < n // 8, height, 1.0)


def together(key, own, strength):
    shared = jax.random.normal(key, own.shape[1:], jnp.float32)
    return (own + strength * shared) * lax.rsqrt(1 + strength * strength)


def setup_inputs(seed: int = 0, part: int = 0) -> dict:
    kx, kdy, ka, kb, kz, kf, kh, kl, *keys = jax.random.split(jax.random.key(seed), 8 + 3 * len(NAMES))
    kx, kdy, ka, kb = (jax.random.fold_in(k, part) for k in (kx, kdy, ka, kb))
    kw, km, kv = (keys[i::3] for i in range(3))
    shape = (SEQUENCES, TOKENS, D)
    much_x, much_dy = jax.random.uniform(kz, (2,), jnp.float32, 0.0, 1.0)
    loud = 2.0 ** jax.random.uniform(jax.random.fold_in(kz, 1), (), jnp.float32, -1.0, 2.0)
    layers = 2.0 ** jax.random.uniform(kl, (LAYERS, 1, 1), jnp.float32, -1.0, 1.0)
    x = together(ka, jax.random.normal(kx, shape, jnp.float32), much_x) * bump(kf, D, 4.0)
    dy = together(kb, jax.random.normal(kdy, shape, jnp.float32), much_dy)
    drawn = {"x": x.astype(jnp.bfloat16), "dy": (loud * dy * (SEQUENCES * TOKENS) ** -0.5).astype(jnp.bfloat16)}
    for key, name in zip(kw, NAMES, strict=True):
        w = jax.random.normal(key, SHAPES[name], jnp.float32) * SHAPES[name][1] ** -0.5
        drawn[name] = (w * {"w_gate": 1.0, "w_up": bump(kh, FF, 4.0), "w_down": layers}[name]).astype(jnp.bfloat16)
    for key, name in zip(km, NAMES, strict=True):
        drawn[f"m_{name}"] = 0.1 * jax.random.normal(key, SHAPES[name], jnp.float32)
    for key, name in zip(kv, NAMES, strict=True):
        drawn[f"v_{name}"] = jax.random.uniform(key, SHAPES[name], jnp.float32, 0.005, 0.015)
    return drawn


def matmul(a, w):
    return jnp.dot(a, w, preferred_element_type=jnp.float32).astype(jnp.bfloat16)


def normed(h):
    wide = h.astype(jnp.float32)
    scale = lax.rsqrt(jnp.mean(wide**2, -1, keepdims=True) + 1e-6)
    return (wide * scale).astype(jnp.bfloat16)


def layer(h, w):
    a = normed(h)
    gate = jnp.dot(a, w["w_gate"], preferred_element_type=jnp.float32)
    up = jnp.dot(a, w["w_up"], preferred_element_type=jnp.float32)
    return h + matmul((jax.nn.silu(gate) * up).astype(jnp.bfloat16), w["w_down"])


def adamw(w, m, v, g):
    m = 0.9 * m + 0.1 * g
    v = 0.95 * v + 0.05 * g * g
    step = m * lax.rsqrt(v + 1e-8) + 0.1 * w
    return (w - 0.02 * step).astype(jnp.bfloat16), m, v


def stack(weights, h):
    return lax.scan(lambda h, w: (layer(h, w), None), h, weights)[0]


def reference(x, dy, w_gate, w_up, w_down, m_w_gate, m_w_up, m_w_down, v_w_gate, v_w_up, v_w_down):
    weights = dict(zip(NAMES, (w_gate, w_up, w_down), strict=True))

    def take(so_far, sequence):
        h, by_y = sequence
        _, back = jax.vjp(lambda w: stack(w, h), weights)
        return jax.tree.map(lambda total, term: total + term.astype(jnp.float32), so_far, back(by_y)[0]), None

    none_yet = {name: jnp.zeros(w.shape, jnp.float32) for name, w in weights.items()}
    by_weights, _ = lax.scan(take, none_yet, (x, dy))
    gradients = [by_weights[name].astype(jnp.bfloat16).astype(jnp.float32) for name in NAMES]
    new = [
        adamw(w.astype(jnp.float32), m, v, g)
        for w, m, v, g in zip((w_gate, w_up, w_down), (m_w_gate, m_w_up, m_w_down), (v_w_gate, v_w_up, v_w_down), gradients, strict=True)
    ]
    return tuple(one[which] for which in range(3) for one in new)
```

```python
import functools

import jax
import jax.numpy as jnp
from jax import lax
from jax.experimental import pallas as pl
from jax.experimental.pallas import tpu as pltpu
from jax.sharding import PartitionSpec as P


LANES = 128
FB = 2 * LANES
K1_ROWS = 512
S1_ROWS = 256
DA_ROWS = 512
CHAINS = (4, 3)
SLOTS = 2 * CHAINS[0]
PACE = ((3, 2), (3, 2), (11, 10))
GROUPS = (8, 5, 3)
MIB = 1 << 20
MESH = pl.DeviceIdType.MESH
ANY = pl.BlockSpec(memory_space=pl.ANY)
bf16, f32 = jnp.bfloat16, jnp.float32


def wide(x):
    return x.astype(f32)


def dot(a, b, dims=((1,), (0,))):
    return lax.dot_general(a, b, (dims, ((), ())), preferred_element_type=f32)


def normed(h):
    h = wide(h)
    return (h * lax.rsqrt(jnp.mean(h * h, -1, keepdims=True) + 1e-6)).astype(bf16)


def adamw(w, m, v, g):
    m = 0.9 * m + 0.1 * g
    v = 0.95 * v + 0.05 * g * g
    step = m * lax.rsqrt(v + 1e-8) + 0.1 * w
    return (w - 0.02 * step).astype(bf16), m, v


def forward_kernel(h_ref, dy_ref, wg_ref, wu_ref, wd_ref, h1_ref, a1_ref, a1t_ref, a0_ref, a0t_ref, dyt_ref, act_ref):
    ff = wg_ref.shape[-1]
    a = normed(h_ref[...])
    a0_ref[...] = a
    a0t_ref[...] = a.T
    dyt_ref[...] = dy_ref[...].T
    for f in range(0, ff, FB):
        cols = slice(f, min(f + FB, ff))
        gate, up = dot(a, wg_ref[:, cols]), dot(a, wu_ref[:, cols])
        act_ref[:, cols] = (gate * jax.nn.sigmoid(gate) * up).astype(bf16)
    h1 = h_ref[...] + dot(act_ref[...], wd_ref[...]).astype(bf16)
    h1_ref[...] = h1
    a1 = normed(h1)
    a1_ref[...] = a1
    a1t_ref[...] = a1.T


def forward(x, dy, wg, wu, wd):
    (tokens, d), ff = x.shape, wg.shape[-1]
    rows = pl.BlockSpec((K1_ROWS, d), lambda i: (i, 0))
    cols = pl.BlockSpec((d, K1_ROWS), lambda i: (0, i))
    once = functools.partial(pl.BlockSpec, index_map=lambda i: (0, 0, 0), pipeline_mode=pl.Buffered(1))
    up, across = jax.ShapeDtypeStruct((tokens, d), bf16), jax.ShapeDtypeStruct((d, tokens), bf16)
    return pl.pallas_call(
        forward_kernel,
        out_shape=(up, up, across, up, across, across),
        grid=(tokens // K1_ROWS,),
        in_specs=[rows, rows, once((None, d, ff)), once((None, d, ff)), once((None, ff, d))],
        out_specs=(rows, rows, cols, rows, cols, cols),
        scratch_shapes=[pltpu.VMEM((K1_ROWS, ff), bf16)],
        compiler_params=pltpu.CompilerParams(vmem_limit_bytes=56 * MIB),
        cost_estimate=pl.CostEstimate(flops=6 * tokens * d * ff, bytes_accessed=8 * d * ff, transcendentals=0),
        name="forward0",
    )(x, dy, wg, wu, wd)


def backward_kernel(n, *refs):
    (a1, a1t, dy, dyt, h1, a0, a0t, wg, wu, wd), refs = refs[:10], refs[10:]
    out_refs, refs = refs[: len(GROUPS)], refs[len(GROUPS) :]
    (av, atv, dv, dtv, dgv, duv, actv, wgr, wur, wdr, wgf, wuf, hv, g_ref, ra, rb) = refs[:16]
    (sem_w, sem_in, sem_full, sem_h, sem_sa, sem_ra, sem_sb, sem_rb, free_a, free_b, sem_out) = refs[16:]
    tokens, d = av.shape
    ff = wg.shape[-1]
    units, lanes = g_ref.shape[:2]
    half = lanes // 2
    full = ff // FB
    blocks = full + 1
    rows = d // n
    rounds = n // 2

    me = lax.axis_index("dp")
    right, left = lax.rem(me + 1, n), lax.rem(me + n - 1, n)

    def shard(s):
        return pl.ds(pl.multiple_of(lax.rem(s, n) * rows, 16), rows)

    c1, c2 = CHAINS
    early, total = full * rounds, units * rounds

    def unit(q):
        e = q - early
        return jnp.where(q < early, q // (rounds * c1) * c1 + lax.rem(q, c1), full + e // (rounds * c2) * c2 + lax.rem(e, c2))

    def turn(q):
        return jnp.where(q < early, lax.rem(q, rounds * c1) // c1, lax.rem(q - early, rounds * c2) // c2)

    def valid(q):
        return jnp.logical_and(q >= 0, q < total)

    def copies(q, both):
        u, r, s = unit(q), turn(q), lax.rem(q, SLOTS)
        ca, cb = (pl.ds(0, lanes),) * 2 if both else (pl.ds(0, half), pl.ds(half, half))
        return (
            pltpu.make_async_remote_copy(
                g_ref.at[u, ca, shard(me + rounds - r)], ra.at[s, ca], sem_sa.at[s], sem_ra.at[s],
                device_id={"dp": right}, device_id_type=MESH,
            ),
            pltpu.make_async_remote_copy(
                g_ref.at[u, cb, shard(me + n - rounds + r)], rb.at[s, cb], sem_sb.at[s], sem_rb.at[s],
                device_id={"dp": left}, device_id_type=MESH,
            ),
        )

    def each(q, what):
        r = turn(q)

        @pl.when(r == 0)
        def _():
            for copy in copies(q, False):
                what(copy)

        @pl.when(r > 0)
        def _():
            for copy in copies(q, True):
                what(copy)

    def send(q):
        @pl.when(valid(q))
        def _():
            @pl.when(valid(q - SLOTS))
            def _():
                pl.semaphore_wait(free_a, 1)
                pl.semaphore_wait(free_b, 1)
                each(q - SLOTS, lambda c: c.wait_send())

            each(q, lambda c: c.start())

    def own(u, what):
        first = 0
        for out in out_refs:

            @pl.when(jnp.logical_and(u >= first, u < first + out.shape[0]))
            def _(out=out, first=first):
                what(pltpu.make_async_copy(g_ref.at[u, :, shard(me)], out.at[u - first], sem_out.at[u]))

            first += out.shape[0]

    def serve(q):
        @pl.when(valid(q))
        def _():
            u, r, s = unit(q), turn(q), lax.rem(q, SLOTS)
            at, bt = shard(me + rounds - 1 - r), shard(me + n - rounds + 1 + r)
            each(q, lambda c: c.wait_recv())

            @pl.when(r == 0)
            def _():
                g_ref[u, :half, at] = (wide(g_ref[u, :half, at]) + wide(ra[s, :half])).astype(bf16)
                g_ref[u, half:, bt] = (wide(g_ref[u, half:, bt]) + wide(rb[s, half:])).astype(bf16)

            @pl.when(jnp.logical_and(r > 0, r < rounds - 1))
            def _():
                g_ref[u, :, at] = (wide(g_ref[u, :, at]) + wide(ra[s])).astype(bf16)
                g_ref[u, :, bt] = (wide(g_ref[u, :, bt]) + wide(rb[s])).astype(bf16)

            @pl.when(r == rounds - 1)
            def _():
                g_ref[u, :, at] = (wide(g_ref[u, :, at]) + wide(ra[s]) + wide(rb[s])).astype(bf16)

            @pl.when(valid(q + SLOTS))
            def _():
                pl.semaphore_signal(free_a, inc=1, device_id={"dp": left}, device_id_type=MESH)
                pl.semaphore_signal(free_b, inc=1, device_id={"dp": right}, device_id_type=MESH)

            @pl.when(r == rounds - 1)
            def _():
                own(u, lambda c: c.start())

        @pl.when(q < early - 1)
        def _():
            send(q + c1)

        @pl.when(q >= early)
        def _():
            send(q + c2)

    def serve_all(first, last):
        def one(q, carry):
            serve(q)
            return carry

        lax.fori_loop(first, last, one, 0)

    def paced(pace, k):
        return k * pace[0] // pace[1]

    ends = (c1 - 1) + paced(PACE[0], 2 * (blocks - c1)), 0
    ends = ends[0], ends[0] + paced(PACE[1], tokens // DA_ROWS)
    finish = ends[1] + paced(PACE[2], 2 * blocks)

    def served(b, i):
        later = b - blocks
        return jnp.where(
            b < blocks, c1 - 1 + paced(PACE[0], 2 * (b - c1) + i + 1), ends[1] + paced(PACE[2], 2 * later + i + 1)
        )

    def point(b, i):
        if i == 1:

            @pl.when(b < c1)
            def _():
                send(b)

                @pl.when(b > 0)
                def _():
                    serve(b - 1)

        @pl.when(b >= c1)
        def _():
            serve_all(served(b, i - 1), served(b, i))

    loads = [
        pltpu.make_async_copy(src, dst, sem_in.at[i])
        for i, (src, dst) in enumerate(((a1, av), (dy, dv), (a1t, atv), (dyt, dtv)))
    ]
    second = [pltpu.make_async_copy(src, dst, sem_in.at[i]) for i, (src, dst) in enumerate(((a0, av), (a0t, atv)))]
    whole = [pltpu.make_async_copy(src.at[1], dst, sem_full.at[i]) for i, (src, dst) in enumerate(((wg, wgf), (wu, wuf)))]

    def place(b):
        layer = jnp.where(b < blocks, 1, 0)
        j = jnp.where(b < blocks, b, b - blocks)
        return layer, j, pl.multiple_of(jnp.minimum(j * FB, ff - FB), LANES)

    def weights(b):
        layer, _, c = place(b)
        s = lax.rem(b, 2)
        return (
            pltpu.make_async_copy(wg.at[layer, :, pl.ds(c, FB)], wgr.at[s], sem_w.at[0, s]),
            pltpu.make_async_copy(wu.at[layer, :, pl.ds(c, FB)], wur.at[s], sem_w.at[1, s]),
            pltpu.make_async_copy(wd.at[layer, pl.ds(c, FB), :], wdr.at[s], sem_w.at[2, s]),
        )

    for copy in (*weights(jnp.int32(0)), *loads[:2]):
        copy.start()
    barrier = pltpu.get_barrier_semaphore()
    for neighbour in (left, right):
        pl.semaphore_signal(barrier, inc=1, device_id={"dp": neighbour}, device_id_type=MESH)
    for copy in loads[2:]:
        copy.start()
    for copy in loads[:2]:
        copy.wait()
    pl.semaphore_wait(barrier, 2)

    def h_tile(t):
        return pltpu.make_async_copy(h1.at[pl.ds(t * DA_ROWS, DA_ROWS)], hv.at[lax.rem(t, 2)], sem_h.at[lax.rem(t, 2)])

    def through_norm():
        da_tiles = tokens // DA_ROWS
        for copy in second:
            copy.start()
        for copy in whole:
            copy.wait()
        h_tile(jnp.int32(0)).start()

        def tile(t, carry):
            r = pl.ds(pl.multiple_of(t * DA_ROWS, DA_ROWS), DA_ROWS)

            @pl.when(t + 1 < da_tiles)
            def _():
                h_tile(t + 1).start()

            h_tile(t).wait()
            last = ((1,), (1,))
            da = wide(dot(dgv[r, :], wgf[...], last).astype(bf16)) + wide(dot(duv[r, :], wuf[...], last).astype(bf16))
            da = wide(da.astype(bf16))
            h = wide(hv[lax.rem(t, 2)])
            scale = lax.rsqrt(jnp.mean(h * h, -1, keepdims=True) + 1e-6)
            dh = (da * scale - h * (scale * scale * scale * jnp.mean(da * h, -1, keepdims=True))).astype(bf16)
            dh = (wide(dv[r, :]) + wide(dh)).astype(bf16)
            dv[r, :] = dh
            dtv[:, r] = dh.T
            serve_all(ends[0] + paced(PACE[1], t), ends[0] + paced(PACE[1], t + 1))
            return carry

        lax.fori_loop(0, da_tiles, tile, 0)
        for copy in second:
            copy.wait()

    def block(b, carry):
        layer, j, c = place(b)
        s = lax.rem(b, 2)
        cols = pl.ds(c, FB)
        for copy in weights(b):
            copy.wait()

        @pl.when(b + 1 < 2 * blocks)
        def _():
            for copy in weights(b + 1):
                copy.start()

        @pl.when(b == 1)
        def _():
            for copy in whole:
                copy.start()

        @pl.when(b == blocks)
        def _():
            through_norm()

        def products(r):
            return dot(av[r, :], wgr[s]), dot(av[r, :], wur[s]), dot(dv[r, :], wdr[s], ((1,), (1,)))

        def pointwise(r, gate, up, dact):
            dact = wide(dact.astype(bf16))
            sig = jax.nn.sigmoid(gate)
            silu = gate * sig
            actv[r, :] = (silu * up).astype(bf16)
            duv[r, cols] = (dact * silu).astype(bf16)
            dgv[r, cols] = (dact * up * (sig + silu * (1.0 - sig))).astype(bf16)

        before = None
        for t in range(tokens // S1_ROWS):
            r = slice(t * S1_ROWS, (t + 1) * S1_ROWS)
            made = products(r)
            if before is not None:
                pointwise(*before)
            before = (r, *made)
        pointwise(*before)
        point(b, 0)

        @pl.when(b == 0)
        def _():
            for copy in loads[2:]:
                copy.wait()

        rest = j == full
        u = jnp.where(rest, units - 1, jnp.where(layer == 1, j, full + j))
        h0, h1_ = jnp.where(rest, 1 - layer, 0), jnp.where(rest, 1 - layer, 1)
        dwg = dot(atv[...], dgv[:, cols]).astype(bf16)
        dwu = dot(atv[...], duv[:, cols]).astype(bf16)
        dwd = dot(dtv[...], actv[...]).astype(bf16)
        for h, k in ((h0, 0), (h1_, LANES)):
            g_ref[u, h] = dwg[:, k : k + LANES]
            g_ref[u, half + h] = dwu[:, k : k + LANES]
            g_ref[u, half - 1 + half * h] = dwd[:, k : k + LANES]
        point(b, 1)
        return carry

    lax.fori_loop(0, 2 * blocks, block, 0)
    serve_all(finish, total)

    def sent(q, carry):
        each(q, lambda c: c.wait_send())
        return carry

    lax.fori_loop(total - SLOTS, total, sent, 0)

    def written(u, carry):
        own(u, lambda c: c.wait())
        return carry

    lax.fori_loop(0, units, written, 0)


def backward(n, a1, a1t, dy, dyt, h1, a0, a0t, wg, wu, wd):
    (tokens, d), (layers, _, ff) = a1.shape, wg.shape
    units, lanes = layers * (ff // FB) + 1, 3 * FB // LANES
    assert layers == 2 and ff % FB == LANES and d % (16 * n) == 0 and sum(GROUPS) + 1 == units
    assert (ff // FB) % CHAINS[0] == 0 and (units - ff // FB) % CHAINS[1] == 0
    sizes = (*GROUPS[:-1], GROUPS[-1] + 1)
    dma, vmem = pltpu.SemaphoreType.DMA, lambda *shape: pltpu.VMEM(shape, bf16)
    return pl.pallas_call(
        functools.partial(backward_kernel, n),
        out_shape=tuple(jax.ShapeDtypeStruct((size, lanes, d // n, LANES), bf16) for size in sizes),
        in_specs=[ANY] * 10,
        out_specs=(ANY,) * len(sizes),
        scratch_shapes=[
            vmem(tokens, d), vmem(d, tokens), vmem(tokens, d), vmem(d, tokens), vmem(tokens, ff), vmem(tokens, ff),
            vmem(tokens, FB), vmem(2, d, FB), vmem(2, d, FB), vmem(2, FB, d), vmem(d, ff), vmem(d, ff),
            vmem(2, DA_ROWS, d), vmem(units, lanes, d, LANES),
            vmem(SLOTS, lanes, d // n, LANES), vmem(SLOTS, lanes, d // n, LANES),
            dma((3, 2)), dma((4,)), dma((2,)), dma((2,)), dma((SLOTS,)), dma((SLOTS,)), dma((SLOTS,)), dma((SLOTS,)),
            pltpu.SemaphoreType.REGULAR, pltpu.SemaphoreType.REGULAR, dma((units,)),
        ],
        compiler_params=pltpu.CompilerParams(collective_id=0, has_side_effects=True, vmem_limit_bytes=67043328),
        cost_estimate=pl.CostEstimate(flops=24 * tokens * d * ff, bytes_accessed=40 * d * ff, transcendentals=0),
        name="backward_reduce",
    )(a1, a1t, dy, dyt, h1, a0, a0t, wg, wu, wd)


def gather(n, mine):
    right, left = [(i, (i + 1) % n) for i in range(n)], [(i, (i - 1) % n) for i in range(n)]
    shards, from_left, from_right = [(0, mine)], mine, mine
    for r in range(1, n // 2):
        from_left, from_right = lax.ppermute(from_left, "dp", right), lax.ppermute(from_right, "dp", left)
        shards += [(n - r, from_left), (r, from_right)]
    half = mine.shape[1] // 2
    return shards, (lax.ppermute(from_left[:, :half], "dp", right), lax.ppermute(from_right[:, half:], "dp", left))


def adamw_kernel(n, width, aliased, me_ref, *refs):
    shards, (g_lo, g_hi) = refs[: n - 1], refs[n - 1 : n + 1]
    ins, outs, down = refs[n + 1 : n + 10], refs[n + 10 + 9 * aliased : n + 19 + 9 * aliased], refs[-1]
    w, m, v = ins[:3], ins[3:6], ins[6:]
    rows = shards[0].shape[-2]
    lanes = shards[0].shape[1]
    half = lanes // 2
    me = me_ref[0]
    offsets = [0] + [s for r in range(1, n // 2) for s in (n - r, r)]
    parts = [(o, lambda k, b=b: b[0, k]) for o, b in zip(offsets, shards, strict=True)]
    parts.append((n // 2, lambda k: g_lo[0, k] if k < half else g_hi[0, k - half]))
    for offset, lane in parts:
        at = pl.ds(pl.multiple_of(lax.rem(me + offset, n) * rows, 16), rows)
        for k in range(width // LANES):
            cols = slice(k * LANES, (k + 1) * LANES)
            if width == FB:
                picked = [lane(k), lane(half + k), lane(half - 1 + half * k)]
            else:
                first = pl.program_id(0) == 0
                picked = [jnp.where(first, lane(i), lane(j)) for i, j in ((0, 1), (half, half + 1), (half - 1, lanes - 1))]
            for i in range(2):
                new = adamw(wide(w[i][at, cols]), m[i][at, cols], v[i][at, cols], wide(picked[i]))
                for out, value in zip(outs[i::3], new, strict=True):
                    out[at, cols] = value
            down[at, cols] = wide(picked[2])
    new = adamw(wide(w[2][...]), m[2][...], v[2][...], down[...].T)
    for out, value in zip(outs[2::3], new, strict=True):
        out[...] = value


def optimizer(n, me, shards, halves, start, units, first_unit, arrays, before):
    mine = shards[0][1]
    _, lanes, rows, _ = mine.shape
    layers, d, ff = arrays[0].shape
    full = ff // FB
    mixed = first_unit == layers * full
    width = LANES if mixed else FB
    if mixed:
        place = lambda i: (1 - i, full * (FB // LANES))
        of = lambda i: start
        grid = layers
    else:
        place = lambda i: (1 - (first_unit + i) // full, (first_unit + i) % full)
        of = lambda i: start + i
        grid = units
    up = pl.BlockSpec((None, d, width), lambda i, _: (place(i)[0], 0, place(i)[1]))
    down = pl.BlockSpec((None, width, d), lambda i, _: (place(i)[0], place(i)[1], 0))
    spec = [up, up, down] * 3
    g = [pl.BlockSpec((1, lanes, rows, LANES), lambda i, _: (of(i), 0, 0, 0))] * (n - 1)
    g += [pl.BlockSpec((1, lanes // 2, rows, LANES), lambda i, _: (of(i), 0, 0, 0))] * 2
    shapes = tuple(jax.ShapeDtypeStruct(a.shape, a.dtype) for a in arrays)
    old = () if before is None else before
    return pl.pallas_call(
        functools.partial(adamw_kernel, n, width, bool(old)),
        out_shape=shapes,
        grid_spec=pltpu.PrefetchScalarGridSpec(
            num_scalar_prefetch=1, grid=(grid,), in_specs=g + spec + [ANY] * len(old), out_specs=tuple(spec),
            scratch_shapes=[pltpu.VMEM((d, width), f32)],
        ),
        input_output_aliases={n + 11 + i: i for i in range(len(old))},
        compiler_params=pltpu.CompilerParams(vmem_limit_bytes=48 * MIB),
        cost_estimate=pl.CostEstimate(
            flops=grid * width * d * 3 * 4000, bytes_accessed=grid * width * d * 3 * 22, transcendentals=0
        ),
        name=f"adamw_{first_unit}",
    )(me, *(b for _, b in shards), *halves, *arrays, *old)


def solution(mesh):
    n = mesh.shape["dp"]

    def step(x, dy, *arrays):
        wg, wu, wd = arrays[:3]
        x, dy = x[0], dy[0]
        h1, a1, a1t, a0, a0t, dyt = forward(x, dy, wg, wu, wd)
        reduced = backward(n, a1, a1t, dy, dyt, h1, a0, a0t, wg, wu, wd)
        me = lax.axis_index("dp").astype(jnp.int32)[None]
        new, at = None, 0
        for size, mine in zip(GROUPS, reduced, strict=True):
            gathered = gather(n, mine)
            new = optimizer(n, me, *gathered, 0, size, at, arrays, new)
            at += size
            if mine.shape[0] > size:
                new = optimizer(n, me, *gathered, size, 1, at, arrays, new)
        return new

    return jax.shard_map(
        step,
        mesh=mesh,
        in_specs=(P(("rep", "dp"), None, None),) * 2 + (P(None, None, None),) * 9,
        out_specs=(P("rep", None, None),) * 9,
        check_vma=False,
    )
```

```python
import functools

import jax
import jax.numpy as jnp
from jax import lax
from jax.experimental import pallas as pl
from jax.experimental.pallas import tpu as pltpu
from jax.sharding import PartitionSpec as P


LANES = 128
FB = 2 * LANES
K1_ROWS = 512
S1_ROWS = 256
DA_ROWS = 512
STAGGER = 2
LEAD = 2
SLOTS = 12
S1_PARTS = 1
POINTS = S1_PARTS + 1
ALONE = 4
PACE = ((15, 10), (3, 2), (4, 3))
MIB = 1 << 20
MESH = pl.DeviceIdType.MESH
ANY = pl.BlockSpec(memory_space=pl.ANY)
bf16, f32 = jnp.bfloat16, jnp.float32


def wide(x):
    return x.astype(f32)


def dot(a, b, dims=((1,), (0,))):
    return lax.dot_general(a, b, (dims, ((), ())), preferred_element_type=f32)


def normed(h):
    h = wide(h)
    return (h * lax.rsqrt(jnp.mean(h * h, -1, keepdims=True) + 1e-6)).astype(bf16)


def adamw(w, m, v, g):
    m = 0.9 * m + 0.1 * g
    v = 0.95 * v + 0.05 * g * g
    step = m * lax.rsqrt(v + 1e-8) + 0.1 * w
    return (w - 0.02 * step).astype(bf16), m, v


def forward_kernel(h_ref, wg_ref, wu_ref, wd_ref, h1_ref, a1_ref, a1t_ref, a0_ref, a0t_ref, act_ref):
    ff = wg_ref.shape[-1]
    a = normed(h_ref[...])
    a0_ref[...] = a
    a0t_ref[...] = a.T
    for f in range(0, ff, FB):
        cols = slice(f, min(f + FB, ff))
        gate, up = dot(a, wg_ref[:, cols]), dot(a, wu_ref[:, cols])
        act_ref[:, cols] = (gate * jax.nn.sigmoid(gate) * up).astype(bf16)
    h1 = h_ref[...] + dot(act_ref[...], wd_ref[...]).astype(bf16)
    h1_ref[...] = h1
    a1 = normed(h1)
    a1_ref[...] = a1
    a1t_ref[...] = a1.T


def forward(x, wg, wu, wd):
    (tokens, d), ff = x.shape, wg.shape[-1]
    rows = pl.BlockSpec((K1_ROWS, d), lambda i: (i, 0))
    cols = pl.BlockSpec((d, K1_ROWS), lambda i: (0, i))
    once = functools.partial(pl.BlockSpec, index_map=lambda i: (0, 0, 0), pipeline_mode=pl.Buffered(1))
    up, across = jax.ShapeDtypeStruct((tokens, d), bf16), jax.ShapeDtypeStruct((d, tokens), bf16)
    return pl.pallas_call(
        forward_kernel,
        out_shape=(up, up, across, up, across),
        grid=(tokens // K1_ROWS,),
        in_specs=[rows, once((None, d, ff)), once((None, d, ff)), once((None, ff, d))],
        out_specs=(rows, rows, cols, rows, cols),
        scratch_shapes=[pltpu.VMEM((K1_ROWS, ff), bf16)],
        compiler_params=pltpu.CompilerParams(vmem_limit_bytes=56 * MIB),
        cost_estimate=pl.CostEstimate(flops=6 * tokens * d * ff, bytes_accessed=8 * d * ff, transcendentals=0),
        name="forward0",
    )(x, wg, wu, wd)


def backward_kernel(n, *refs):
    (a1, a1t, dy, h1, a0, a0t, wg, wu, wd, *out_refs), refs = refs[:11], refs[11:]
    (av, atv, dv, dgv, duv, actv, wgr, wur, wdr, wgf, wuf, hv, g_ref, ra, rb) = refs[:15]
    (sem_w, sem_in, sem_full, sem_h, sem_sa, sem_ra, sem_sb, sem_rb, free_a, free_b, sem_out) = refs[15:]
    tokens, d = av.shape
    ff = wg.shape[-1]
    units, lanes = g_ref.shape[:2]
    half = lanes // 2
    full = ff // FB
    blocks = full + 1
    rows = d // n
    rounds = n // 2

    me = lax.axis_index("dp")
    right, left = lax.rem(me + 1, n), lax.rem(me + n - 1, n)

    def shard(s):
        return pl.ds(pl.multiple_of(lax.rem(s, n) * rows, 16), rows)

    total = (units + STAGGER * (rounds - 1)) * rounds

    def turn(q):
        return rounds - 1 - lax.rem(q, rounds)

    def unit(q):
        return q // rounds - STAGGER * turn(q)

    def valid(q):
        return jnp.logical_and(q >= 0, jnp.logical_and(unit(q) >= 0, unit(q) < units))

    def copies(q, both):
        u, r, s = unit(q), turn(q), lax.rem(q, SLOTS)
        ca, cb = (pl.ds(0, lanes),) * 2 if both else (pl.ds(0, half), pl.ds(half, half))
        return (
            pltpu.make_async_remote_copy(
                g_ref.at[u, ca, shard(me + rounds - r)], ra.at[s, ca], sem_sa.at[s], sem_ra.at[s],
                device_id={"dp": right}, device_id_type=MESH,
            ),
            pltpu.make_async_remote_copy(
                g_ref.at[u, cb, shard(me + n - rounds + r)], rb.at[s, cb], sem_sb.at[s], sem_rb.at[s],
                device_id={"dp": left}, device_id_type=MESH,
            ),
        )

    def each(q, what):
        r = turn(q)

        @pl.when(r == 0)
        def _():
            for copy in copies(q, False):
                what(copy)

        @pl.when(r > 0)
        def _():
            for copy in copies(q, True):
                what(copy)

    def send(q):
        @pl.when(valid(q))
        def _():
            @pl.when(valid(q - SLOTS))
            def _():
                pl.semaphore_wait(free_a.at[lax.rem(q, SLOTS)], 1)
                pl.semaphore_wait(free_b.at[lax.rem(q, SLOTS)], 1)
                each(q - SLOTS, lambda c: c.wait_send())

            each(q, lambda c: c.start())

    def own(u, what):
        def to(out, k):
            what(pltpu.make_async_copy(g_ref.at[u, :, shard(me)], out.at[k], sem_out.at[u]))

        @pl.when(u < full)
        def _():
            to(out_refs[0], u)

        @pl.when(u == units - 1)
        def _():
            to(out_refs[0], full)

        @pl.when(jnp.logical_and(u >= full, u < units - 1))
        def _():
            to(out_refs[1], u - full)

    def start(u):
        send(u * rounds + rounds - 1)

    def serve(q, ready):
        @pl.when(valid(q))
        def _():
            u, r, s = unit(q), turn(q), lax.rem(q, SLOTS)
            at, bt = shard(me + rounds - 1 - r), shard(me + n - rounds + 1 + r)
            each(q, lambda c: c.wait_recv())

            @pl.when(r == 0)
            def _():
                g_ref[u, :half, at] = (wide(g_ref[u, :half, at]) + wide(ra[s, :half])).astype(bf16)
                g_ref[u, half:, bt] = (wide(g_ref[u, half:, bt]) + wide(rb[s, half:])).astype(bf16)

            @pl.when(jnp.logical_and(r > 0, r < rounds - 1))
            def _():
                g_ref[u, :, at] = (wide(g_ref[u, :, at]) + wide(ra[s])).astype(bf16)
                g_ref[u, :, bt] = (wide(g_ref[u, :, bt]) + wide(rb[s])).astype(bf16)

            @pl.when(r == rounds - 1)
            def _():
                g_ref[u, :, at] = (wide(g_ref[u, :, at]) + wide(ra[s]) + wide(rb[s])).astype(bf16)

            @pl.when(valid(q + SLOTS))
            def _():
                pl.semaphore_signal(free_a.at[s], inc=1, device_id={"dp": left}, device_id_type=MESH)
                pl.semaphore_signal(free_b.at[s], inc=1, device_id={"dp": right}, device_id_type=MESH)

            @pl.when(r == rounds - 1)
            def _():
                own(u, lambda c: c.start())

            @pl.when(r < rounds - 1)
            def _():
                send(q + STAGGER * rounds - 1)

            @pl.when(jnp.logical_and(r == 0, u + LEAD < ready))
            def _():
                start(u + LEAD)

    def serve_all(first, last, ready):
        def one(q, carry):
            serve(q, ready)
            return carry

        lax.fori_loop(first, last, one, 0)

    def paced(pace, k):
        return k * pace[0] // pace[1]

    first = (ALONE - 1) * rounds + paced(PACE[0], POINTS * (blocks - ALONE))
    later = first + paced(PACE[1], tokens // DA_ROWS)
    finish = later + paced(PACE[2], POINTS * blocks)

    def served(b, i):
        regular = jnp.where(
            b < blocks,
            (ALONE - 1) * rounds + paced(PACE[0], POINTS * (b - ALONE) + i + 1),
            later + paced(PACE[2], POINTS * (b - blocks) + i + 1),
        )
        alone = jnp.maximum(b - 1 + (i == POINTS - 1), 0) * rounds
        return jnp.where(b < ALONE, alone, regular)

    def ready(b):
        return jnp.where(b < blocks, jnp.minimum(b, full), b - 1)

    def point(b, i):
        if i < POINTS - 1:
            serve_all(served(b, i - 1), served(b, i), ready(b))
            return
        made = ready(b + 1)
        u = made - 1

        @pl.when(jnp.logical_and(made > ready(b), jnp.logical_or(u < LEAD, served(b, i - 1) >= (u - LEAD + 1) * rounds)))
        def _():
            start(u)

        serve_all(served(b, i - 1), served(b, i), made)

    loads = [
        pltpu.make_async_copy(src, dst, sem_in.at[i])
        for i, (src, dst) in enumerate(((a1, av), (dy, dv), (a1t, atv)))
    ]
    second = [pltpu.make_async_copy(src, dst, sem_in.at[i]) for i, (src, dst) in enumerate(((a0, av), (a0t, atv)))]
    whole = [pltpu.make_async_copy(src.at[1], dst, sem_full.at[i]) for i, (src, dst) in enumerate(((wg, wgf), (wu, wuf)))]

    def place(b):
        layer = jnp.where(b < blocks, 1, 0)
        j = jnp.where(b < blocks, b, b - blocks)
        return layer, j, pl.multiple_of(jnp.minimum(j * FB, ff - FB), LANES)

    def weights(b):
        layer, _, c = place(b)
        s = lax.rem(b, 2)
        return (
            pltpu.make_async_copy(wg.at[layer, :, pl.ds(c, FB)], wgr.at[s], sem_w.at[0, s]),
            pltpu.make_async_copy(wu.at[layer, :, pl.ds(c, FB)], wur.at[s], sem_w.at[1, s]),
            pltpu.make_async_copy(wd.at[layer, pl.ds(c, FB), :], wdr.at[s], sem_w.at[2, s]),
        )

    for copy in (*weights(jnp.int32(0)), *loads[:2]):
        copy.start()
    barrier = pltpu.get_barrier_semaphore()
    for neighbour in (left, right):
        pl.semaphore_signal(barrier, inc=1, device_id={"dp": neighbour}, device_id_type=MESH)
    for copy in loads[2:]:
        copy.start()
    for copy in loads[:2]:
        copy.wait()
    pl.semaphore_wait(barrier, 2)

    def h_tile(t):
        return pltpu.make_async_copy(h1.at[pl.ds(t * DA_ROWS, DA_ROWS)], hv.at[lax.rem(t, 2)], sem_h.at[lax.rem(t, 2)])

    def through_norm():
        da_tiles = tokens // DA_ROWS
        for copy in second:
            copy.start()
        for copy in whole:
            copy.wait()
        h_tile(jnp.int32(0)).start()

        def tile(t, carry):
            r = pl.ds(pl.multiple_of(t * DA_ROWS, DA_ROWS), DA_ROWS)

            @pl.when(t + 1 < da_tiles)
            def _():
                h_tile(t + 1).start()

            h_tile(t).wait()
            last = ((1,), (1,))
            da = wide(dot(dgv[r, :], wgf[...], last).astype(bf16)) + wide(dot(duv[r, :], wuf[...], last).astype(bf16))
            da = wide(da.astype(bf16))
            h = wide(hv[lax.rem(t, 2)])
            scale = lax.rsqrt(jnp.mean(h * h, -1, keepdims=True) + 1e-6)
            dh = (da * scale - h * (scale * scale * scale * jnp.mean(da * h, -1, keepdims=True))).astype(bf16)
            dh = (wide(dv[r, :]) + wide(dh)).astype(bf16)
            dv[r, :] = dh
            serve_all(first + paced(PACE[1], t), first + paced(PACE[1], t + 1), full)
            return carry

        lax.fori_loop(0, da_tiles, tile, 0)
        for copy in second:
            copy.wait()

    def block(b, carry):
        layer, j, c = place(b)
        s = lax.rem(b, 2)
        cols = pl.ds(c, FB)
        for copy in weights(b):
            copy.wait()

        @pl.when(b + 1 < 2 * blocks)
        def _():
            for copy in weights(b + 1):
                copy.start()

        @pl.when(b == 1)
        def _():
            for copy in whole:
                copy.start()

        @pl.when(b == blocks)
        def _():
            through_norm()

        def products(r):
            return dot(av[r, :], wgr[s]), dot(av[r, :], wur[s]), dot(dv[r, :], wdr[s], ((1,), (1,)))

        def pointwise(r, gate, up, dact):
            dact = wide(dact.astype(bf16))
            sig = jax.nn.sigmoid(gate)
            silu = gate * sig
            actv[r, :] = (silu * up).astype(bf16)
            duv[r, cols] = (dact * silu).astype(bf16)
            dgv[r, cols] = (dact * up * (sig + silu * (1.0 - sig))).astype(bf16)

        for i in range(S1_PARTS):
            before = None
            for t in range(tokens // S1_ROWS // S1_PARTS * i, tokens // S1_ROWS // S1_PARTS * (i + 1)):
                r = slice(t * S1_ROWS, (t + 1) * S1_ROWS)
                made = products(r)
                if before is not None:
                    pointwise(*before)
                before = (r, *made)
            pointwise(*before)
            point(b, i)

        @pl.when(b == 0)
        def _():
            for copy in loads[2:]:
                copy.wait()

        rest = j == full
        u = jnp.where(rest, units - 1, jnp.where(layer == 1, j, full + j))
        h0, h1_ = jnp.where(rest, 1 - layer, 0), jnp.where(rest, 1 - layer, 1)
        dwg = dot(atv[...], dgv[:, cols]).astype(bf16)
        dwu = dot(atv[...], duv[:, cols]).astype(bf16)
        dwd = dot(actv[...], dv[...], ((0,), (0,))).astype(bf16)
        for h, k in ((h0, 0), (h1_, LANES)):
            g_ref[u, h] = dwg[:, k : k + LANES]
            g_ref[u, half + h] = dwu[:, k : k + LANES]
            g_ref[u, half - 1 + half * h] = jnp.concatenate(
                [
                    dwd[k + LANES // n * s_ : k + LANES // n * (s_ + 1), c_ : c_ + LANES]
                    for s_ in range(n)
                    for c_ in range(0, d, LANES)
                ],
                0,
            )
        point(b, POINTS - 1)
        return carry

    lax.fori_loop(0, 2 * blocks, block, 0)
    serve_all(finish, total, units)

    def sent(q, carry):
        @pl.when(jnp.logical_and(valid(q), jnp.logical_not(valid(q + SLOTS))))
        def _():
            each(q, lambda c: c.wait_send())

        return carry

    lax.fori_loop(0, total, sent, 0)

    def written(u, carry):
        own(u, lambda c: c.wait())
        return carry

    lax.fori_loop(0, units, written, 0)


def backward(n, a1, a1t, dy, h1, a0, a0t, wg, wu, wd):
    (tokens, d), (layers, _, ff) = a1.shape, wg.shape
    full, lanes = ff // FB, 3 * FB // LANES
    units = layers * full + 1
    assert layers == 2 and ff % FB == LANES and d % (16 * n) == 0 and LANES // n * (d // LANES) == d // n
    assert SLOTS % (n // 2) == 0 and LEAD + 1 <= SLOTS // (n // 2)
    dma, vmem = pltpu.SemaphoreType.DMA, lambda *shape: pltpu.VMEM(shape, bf16)
    return pl.pallas_call(
        functools.partial(backward_kernel, n),
        out_shape=tuple(jax.ShapeDtypeStruct((size, lanes, d // n, LANES), bf16) for size in (full + 1, full)),
        in_specs=[ANY] * 9,
        out_specs=(ANY,) * 2,
        scratch_shapes=[
            vmem(tokens, d), vmem(d, tokens), vmem(tokens, d), vmem(tokens, ff), vmem(tokens, ff),
            vmem(tokens, FB), vmem(2, d, FB), vmem(2, d, FB), vmem(2, FB, d), vmem(d, ff), vmem(d, ff),
            vmem(2, DA_ROWS, d), vmem(units, lanes, d, LANES),
            vmem(SLOTS, lanes, d // n, LANES), vmem(SLOTS, lanes, d // n, LANES),
            dma((3, 2)), dma((3,)), dma((2,)), dma((2,)), dma((SLOTS,)), dma((SLOTS,)), dma((SLOTS,)), dma((SLOTS,)),
            pltpu.SemaphoreType.REGULAR((SLOTS,)), pltpu.SemaphoreType.REGULAR((SLOTS,)), dma((units,)),
        ],
        compiler_params=pltpu.CompilerParams(collective_id=0, has_side_effects=True, vmem_limit_bytes=67043328),
        cost_estimate=pl.CostEstimate(flops=24 * tokens * d * ff, bytes_accessed=40 * d * ff, transcendentals=0),
        name="backward_reduce",
    )(a1, a1t, dy, h1, a0, a0t, wg, wu, wd)


def gather(n, mine):
    right, left = [(i, (i + 1) % n) for i in range(n)], [(i, (i - 1) % n) for i in range(n)]

    def both(to_right, to_left):
        from_left = lax.ppermute(to_right, "dp", right)
        return from_left, lax.ppermute(to_left, "dp", left)

    from_left = from_right = mine
    rounds = [[(0, mine)]]
    for r in range(1, n // 2):
        from_left, from_right = both(from_left, from_right)
        rounds.append([(n - r, from_left), (r, from_right)])
    half = mine.shape[1] // 2
    return [*rounds, [(n // 2, both(from_left[:, :half], from_right[:, half:]))]]


def adamw_kernel(entries, paired, side, counts, aliased, ids_ref, *refs):
    per = 2 if paired else 1
    grads, refs = refs[: entries * per * len(counts)], refs[entries * per * len(counts) :]
    ins, outs = refs[:9], refs[9 + 9 * aliased :]
    w, m, v = ins[:3], ins[3:6], ins[6:]
    fine, steps = w[2].shape[1], w[2].shape[2] // LANES
    lanes = grads[0].shape[1] * per
    half = lanes // 2
    full = counts[0] - (len(counts) == 1)
    places = [(0, unit, h) for unit in range(full) for h in range(2)]
    places.append((len(counts) - 1, full if len(counts) == 1 else 0, side))

    def step(e):
        def part(j, carry):
            rows = pl.ds(pl.multiple_of(j * fine, fine), fine)
            tile = pl.ds(pl.multiple_of(j * LANES, LANES), LANES)

            def lane(source, unit, k):
                refs = grads[(source * entries + e) * per : (source * entries + e + 1) * per]
                return wide(refs[k // half][unit, k % half, rows] if paired else refs[0][unit, k, rows])

            for at, (source, unit, h) in enumerate(places):
                cols = slice(at * LANES, (at + 1) * LANES)
                for i, where, k in ((0, (rows, cols), h), (1, (rows, cols), half + h), (2, (at, slice(None), tile), half - 1 + half * h)):
                    new = adamw(wide(w[i][where]), m[i][where], v[i][where], lane(source, unit, k))
                    for out, value in zip(outs[i::3], new, strict=True):
                        out[where] = value
            return carry

        lax.fori_loop(0, steps, part, 0)

    for e in range(entries):
        pl.when(pl.program_id(0) == e)(functools.partial(step, e))


def optimizer(n, layer, me, shards, mixed, arrays, before):
    paired = isinstance(shards[0][1], tuple)
    flat = lambda many: [a for _, b in many for a in (b if paired else (b,))]
    grads = flat(shards) + (flat(mixed) if mixed else [])
    rows = grads[0].shape[2]
    _, d, ff = arrays[0].shape
    steps = d // LANES
    assert rows % steps == 0 and rows // steps == LANES // n
    fine = rows // steps
    ids = jnp.concatenate([lax.rem(me + o, n) for o, _ in shards])

    def block(array, whole):
        units = array.shape[0]
        if whole:
            return pl.BlockSpec(array.shape, lambda i, _: (0, 0, 0, 0), pipeline_mode=pl.Buffered(1))
        return pl.BlockSpec((1, *array.shape[1:]), lambda i, _: (units - 1, 0, 0, 0), pipeline_mode=pl.Buffered(1))

    per = 2 if paired else 1
    specs = [block(a, k < len(shards) * per) for k, a in enumerate(grads)]
    up = pl.BlockSpec((None, rows, ff), lambda i, ids: (layer, ids[i], 0))
    down = pl.BlockSpec((None, ff // LANES, fine, d), lambda i, ids: (layer, 0, ids[i], 0))
    spec = [up, up, down] * 3
    counts = [shards[0][1][0].shape[0] if paired else shards[0][1].shape[0]] + ([1] if mixed else [])
    old = () if before is None else before
    return pl.pallas_call(
        functools.partial(adamw_kernel, len(shards), paired, 1 - layer, counts, bool(old)),
        out_shape=tuple(jax.ShapeDtypeStruct(a.shape, a.dtype) for a in arrays),
        grid_spec=pltpu.PrefetchScalarGridSpec(
            num_scalar_prefetch=1, grid=(len(shards),), in_specs=specs + spec + [ANY] * len(old), out_specs=tuple(spec)
        ),
        input_output_aliases={1 + len(grads) + 9 + i: i for i in range(len(old))},
        compiler_params=pltpu.CompilerParams(vmem_limit_bytes=60 * MIB),
        cost_estimate=pl.CostEstimate(
            flops=len(shards) * rows * ff * 3 * 4000, bytes_accessed=len(shards) * rows * ff * 3 * 22, transcendentals=0
        ),
        name="adamw",
    )(ids, *grads, *arrays, *old)


def solution(mesh):
    n = mesh.shape["dp"]

    def step(x, dy, *arrays):
        wg, wu, wd = arrays[:3]
        x, dy = x[0], dy[0]
        h1, a1, a1t, a0, a0t = forward(x, wg, wu, wd)
        second, first = backward(n, a1, a1t, dy, h1, a0, a0t, wg, wu, wd)
        me = lax.axis_index("dp").astype(jnp.int32)[None]
        shapes = [a.shape for a in arrays]
        arrays = [a.reshape(a.shape[0], -1, LANES, a.shape[2]) if i % 3 == 2 else a for i, a in enumerate(arrays)]
        new = None
        for of_second, of_first in zip(gather(n, second), gather(n, first), strict=True):
            new = optimizer(n, 1, me, of_second, None, arrays, new)
            new = optimizer(n, 0, me, of_first, of_second, arrays, new)
        return tuple(a.reshape(shape) for a, shape in zip(new, shapes, strict=True))

    return jax.shard_map(
        step,
        mesh=mesh,
        in_specs=(P(("rep", "dp"), None, None),) * 2 + (P(None, None, None),) * 9,
        out_specs=(P("rep", None, None),) * 9,
        check_vma=False,
    )
```

```python
import functools

import jax
import jax.numpy as jnp
from jax import lax
from jax.experimental import pallas as pl
from jax.experimental.pallas import tpu as pltpu
from jax.sharding import PartitionSpec as P


LANES = 128
FB = 2 * LANES
F_ROWS = 512
DOWN_ROWS = 512
S1_ROWS = 256
STAGGER = 2
LEAD = 2
SLOTS = 12
S1_PARTS = 1
POINTS = S1_PARTS + 1
ALONE = 4
PACE = ((15, 10), (3, 2), (4, 3))
MIB = 1 << 20
MESH = pl.DeviceIdType.MESH
ANY = pl.BlockSpec(memory_space=pl.ANY)
bf16, f32 = jnp.bfloat16, jnp.float32


def wide(x):
    return x.astype(f32)


def dot(a, b, dims=((1,), (0,))):
    return lax.dot_general(a, b, (dims, ((), ())), preferred_element_type=f32)


def normed(h):
    h = wide(h)
    return (h * lax.rsqrt(jnp.mean(h * h, -1, keepdims=True) + 1e-6)).astype(bf16)


def adamw(w, m, v, g):
    m = 0.9 * m + 0.1 * g
    v = 0.95 * v + 0.05 * g * g
    step = m * lax.rsqrt(v + 1e-8) + 0.1 * w
    return (w - 0.02 * step).astype(bf16), m, v


def train_kernel(n, *refs):
    (x, dy, wg, wu, wd, *out_refs), refs = refs[:7], refs[7:]
    (av, atv, dv, dgv, duv, actv, wgr, wur, wdr, wgf, wuf, hv, h1v, g_ref, ra, rb) = refs[:16]
    (sem_w, sem_in, sem_down, sem_full, sem_x, sem_sa, sem_ra, sem_sb, sem_rb, free_a, free_b, sem_out) = refs[16:]
    tokens, d = av.shape
    ff = wg.shape[-1]
    units, lanes = g_ref.shape[:2]
    half = lanes // 2
    full = ff // FB
    blocks = full + 1
    rows = d // n
    rounds = n // 2

    me = lax.axis_index("dp")
    right, left = lax.rem(me + 1, n), lax.rem(me + n - 1, n)

    def shard(s):
        return pl.ds(pl.multiple_of(lax.rem(s, n) * rows, 16), rows)

    total = (units + STAGGER * (rounds - 1)) * rounds

    def turn(q):
        return rounds - 1 - lax.rem(q, rounds)

    def unit(q):
        return q // rounds - STAGGER * turn(q)

    def valid(q):
        return jnp.logical_and(q >= 0, jnp.logical_and(unit(q) >= 0, unit(q) < units))

    def copies(q, both):
        u, r, s = unit(q), turn(q), lax.rem(q, SLOTS)
        ca, cb = (pl.ds(0, lanes),) * 2 if both else (pl.ds(0, half), pl.ds(half, half))
        return (
            pltpu.make_async_remote_copy(
                g_ref.at[u, ca, shard(me + rounds - r)], ra.at[s, ca], sem_sa.at[s], sem_ra.at[s],
                device_id={"dp": right}, device_id_type=MESH,
            ),
            pltpu.make_async_remote_copy(
                g_ref.at[u, cb, shard(me + n - rounds + r)], rb.at[s, cb], sem_sb.at[s], sem_rb.at[s],
                device_id={"dp": left}, device_id_type=MESH,
            ),
        )

    def each(q, what):
        r = turn(q)

        @pl.when(r == 0)
        def _():
            for copy in copies(q, False):
                what(copy)

        @pl.when(r > 0)
        def _():
            for copy in copies(q, True):
                what(copy)

    def send(q):
        @pl.when(valid(q))
        def _():
            @pl.when(valid(q - SLOTS))
            def _():
                pl.semaphore_wait(free_a.at[lax.rem(q, SLOTS)], 1)
                pl.semaphore_wait(free_b.at[lax.rem(q, SLOTS)], 1)
                each(q - SLOTS, lambda c: c.wait_send())

            each(q, lambda c: c.start())

    def own(u, what):
        def to(out, k):
            what(pltpu.make_async_copy(g_ref.at[u, :, shard(me)], out.at[k], sem_out.at[u]))

        @pl.when(u < full)
        def _():
            to(out_refs[0], u)

        @pl.when(u == units - 1)
        def _():
            to(out_refs[0], full)

        @pl.when(jnp.logical_and(u >= full, u < units - 1))
        def _():
            to(out_refs[1], u - full)

    def start(u):
        send(u * rounds + rounds - 1)

    def serve(q, ready):
        @pl.when(valid(q))
        def _():
            u, r, s = unit(q), turn(q), lax.rem(q, SLOTS)
            at, bt = shard(me + rounds - 1 - r), shard(me + n - rounds + 1 + r)
            each(q, lambda c: c.wait_recv())

            @pl.when(r == 0)
            def _():
                g_ref[u, :half, at] = (wide(g_ref[u, :half, at]) + wide(ra[s, :half])).astype(bf16)
                g_ref[u, half:, bt] = (wide(g_ref[u, half:, bt]) + wide(rb[s, half:])).astype(bf16)

            @pl.when(jnp.logical_and(r > 0, r < rounds - 1))
            def _():
                g_ref[u, :, at] = (wide(g_ref[u, :, at]) + wide(ra[s])).astype(bf16)
                g_ref[u, :, bt] = (wide(g_ref[u, :, bt]) + wide(rb[s])).astype(bf16)

            @pl.when(r == rounds - 1)
            def _():
                g_ref[u, :, at] = (wide(g_ref[u, :, at]) + wide(ra[s]) + wide(rb[s])).astype(bf16)

            @pl.when(valid(q + SLOTS))
            def _():
                pl.semaphore_signal(free_a.at[s], inc=1, device_id={"dp": left}, device_id_type=MESH)
                pl.semaphore_signal(free_b.at[s], inc=1, device_id={"dp": right}, device_id_type=MESH)

            @pl.when(r == rounds - 1)
            def _():
                own(u, lambda c: c.start())

            @pl.when(r < rounds - 1)
            def _():
                send(q + STAGGER * rounds - 1)

            @pl.when(jnp.logical_and(r == 0, u + LEAD < ready))
            def _():
                start(u + LEAD)

    def serve_all(first, last, ready):
        def one(q, carry):
            serve(q, ready)
            return carry

        lax.fori_loop(first, last, one, 0)

    def paced(pace, k):
        return k * pace[0] // pace[1]

    first = (ALONE - 1) * rounds + paced(PACE[0], POINTS * (blocks - ALONE))
    later = first + paced(PACE[1], tokens // F_ROWS)
    finish = later + paced(PACE[2], POINTS * blocks)

    def served(b, i):
        regular = jnp.where(
            b < blocks,
            (ALONE - 1) * rounds + paced(PACE[0], POINTS * (b - ALONE) + i + 1),
            later + paced(PACE[2], POINTS * (b - blocks) + i + 1),
        )
        alone = jnp.maximum(b - 1 + (i == POINTS - 1), 0) * rounds
        return jnp.where(b < ALONE, alone, regular)

    def ready(b):
        return jnp.where(b < blocks, jnp.minimum(b, full), b - 1)

    def point(b, i):
        if i < POINTS - 1:
            serve_all(served(b, i - 1), served(b, i), ready(b))
            return
        made = ready(b + 1)
        u = made - 1

        @pl.when(jnp.logical_and(made > ready(b), jnp.logical_or(u < LEAD, served(b, i - 1) >= (u - LEAD + 1) * rounds)))
        def _():
            start(u)

        serve_all(served(b, i - 1), served(b, i), made)

    loads = [
        pltpu.make_async_copy(src, dst, sem_in.at[i])
        for i, (src, dst) in enumerate(((wg.at[0], dgv.at[pl.ds(0, d)]), (wu.at[0], dgv.at[pl.ds(d, d)]), (dy, dv)))
    ]
    runs = [(i, f, min(DOWN_ROWS, ff - f)) for i, f in enumerate(range(0, ff, DOWN_ROWS))]
    downs = [
        pltpu.make_async_copy(
            wd.at[0, pl.ds(f, many), pl.ds(c * LANES, LANES)], g_ref.at[i, c, pl.ds(0, many)], sem_down.at[i, c]
        )
        for i, f, many in runs
        for c in range(d // LANES)
    ]
    whole = [pltpu.make_async_copy(src.at[1], dst, sem_full.at[i]) for i, (src, dst) in enumerate(((wg, wgf), (wu, wuf)))]

    def place(b):
        layer = jnp.where(b < blocks, 1, 0)
        j = jnp.where(b < blocks, b, b - blocks)
        return layer, j, pl.multiple_of(jnp.minimum(j * FB, ff - FB), LANES)

    def weights(b):
        layer, _, c = place(b)
        s = lax.rem(b, 2)
        return (
            pltpu.make_async_copy(wg.at[layer, :, pl.ds(c, FB)], wgr.at[s], sem_w.at[0, s]),
            pltpu.make_async_copy(wu.at[layer, :, pl.ds(c, FB)], wur.at[s], sem_w.at[1, s]),
            pltpu.make_async_copy(wd.at[layer, pl.ds(c, FB), :], wdr.at[s], sem_w.at[2, s]),
        )

    def x_tile(t):
        at = pl.ds(pl.multiple_of(t * F_ROWS, F_ROWS), F_ROWS)
        return pltpu.make_async_copy(x.at[at], hv.at[lax.rem(t, 2)], sem_x.at[lax.rem(t, 2)])

    def next_x(t):
        @pl.when(t + 1 < tokens // F_ROWS)
        def _():
            x_tile(t + 1).start()

        x_tile(t).wait()

    tiles = tokens // F_ROWS

    def normalize(t):
        r = pl.ds(pl.multiple_of(t * F_ROWS, F_ROWS), F_ROWS)
        a = normed(h1v[r, :])
        av[r, :] = a
        atv[:, r] = a.T

    def forward(t, carry):
        r = pl.ds(pl.multiple_of(t * F_ROWS, F_ROWS), F_ROWS)
        next_x(t)
        normalize(lax.rem(t + tiles - 1, tiles))
        h = hv[lax.rem(t, 2)]
        a = normed(h)
        for f in range(0, ff, FB):
            cols = slice(f, min(f + FB, ff))
            gate, up = dot(a, dgv[:d, cols]), dot(a, dgv[d : 2 * d, cols])
            duv[:F_ROWS, cols] = (gate * jax.nn.sigmoid(gate) * up).astype(bf16)
        down = sum(
            dot(duv[:F_ROWS, f : f + many], jnp.concatenate([g_ref[i, c, :many] for c in range(d // LANES)], 1))
            for i, f, many in runs
        )
        h = h + down.astype(bf16)
        h1v[r, :] = h
        return carry

    x_tile(jnp.int32(0)).start()
    for copy in (*loads[:2], *downs, loads[2], *weights(jnp.int32(0))):
        copy.start()
    barrier = pltpu.get_barrier_semaphore()
    for neighbour in (left, right):
        pl.semaphore_signal(barrier, inc=1, device_id={"dp": neighbour}, device_id_type=MESH)
    for copy in (*loads[:2], *downs):
        copy.wait()
    lax.fori_loop(0, tiles, forward, 0)
    normalize(tiles - 1)
    loads[2].wait()
    pl.semaphore_wait(barrier, 2)

    def through_norm():
        for copy in whole:
            copy.wait()
        x_tile(jnp.int32(0)).start()

        def tile(t, carry):
            r = pl.ds(pl.multiple_of(t * F_ROWS, F_ROWS), F_ROWS)
            next_x(t)
            a = normed(hv[lax.rem(t, 2)])
            av[r, :] = a
            atv[:, r] = a.T
            last = ((1,), (1,))
            da = wide(dot(dgv[r, :], wgf[...], last).astype(bf16)) + wide(dot(duv[r, :], wuf[...], last).astype(bf16))
            da = wide(da.astype(bf16))
            h = wide(h1v[r, :])
            scale = lax.rsqrt(jnp.mean(h * h, -1, keepdims=True) + 1e-6)
            dh = (da * scale - h * (scale * scale * scale * jnp.mean(da * h, -1, keepdims=True))).astype(bf16)
            dh = (wide(dv[r, :]) + wide(dh)).astype(bf16)
            dv[r, :] = dh
            serve_all(first + paced(PACE[1], t), first + paced(PACE[1], t + 1), full)
            return carry

        lax.fori_loop(0, tokens // F_ROWS, tile, 0)

    def block(b, carry):
        layer, j, c = place(b)
        s = lax.rem(b, 2)
        cols = pl.ds(c, FB)
        for copy in weights(b):
            copy.wait()

        @pl.when(b + 1 < 2 * blocks)
        def _():
            for copy in weights(b + 1):
                copy.start()

        @pl.when(b == 1)
        def _():
            for copy in whole:
                copy.start()

        @pl.when(b == blocks)
        def _():
            through_norm()

        def products(r):
            return dot(av[r, :], wgr[s]), dot(av[r, :], wur[s]), dot(dv[r, :], wdr[s], ((1,), (1,)))

        def pointwise(r, gate, up, dact):
            dact = wide(dact.astype(bf16))
            sig = jax.nn.sigmoid(gate)
            silu = gate * sig
            actv[r, :] = (silu * up).astype(bf16)
            duv[r, cols] = (dact * silu).astype(bf16)
            dgv[r, cols] = (dact * up * (sig + silu * (1.0 - sig))).astype(bf16)

        for i in range(S1_PARTS):
            before = None
            for t in range(tokens // S1_ROWS // S1_PARTS * i, tokens // S1_ROWS // S1_PARTS * (i + 1)):
                r = slice(t * S1_ROWS, (t + 1) * S1_ROWS)
                made = products(r)
                if before is not None:
                    pointwise(*before)
                before = (r, *made)
            pointwise(*before)
            point(b, i)

        rest = j == full
        u = jnp.where(rest, units - 1, jnp.where(layer == 1, j, full + j))
        h0, h1_ = jnp.where(rest, 1 - layer, 0), jnp.where(rest, 1 - layer, 1)
        dwg = dot(atv[...], dgv[:, cols]).astype(bf16)
        dwu = dot(atv[...], duv[:, cols]).astype(bf16)
        dwd = dot(actv[...], dv[...], ((0,), (0,))).astype(bf16)
        for h, k in ((h0, 0), (h1_, LANES)):
            g_ref[u, h] = dwg[:, k : k + LANES]
            g_ref[u, half + h] = dwu[:, k : k + LANES]
            g_ref[u, half - 1 + half * h] = jnp.concatenate(
                [
                    dwd[k + LANES // n * s_ : k + LANES // n * (s_ + 1), c_ : c_ + LANES]
                    for s_ in range(n)
                    for c_ in range(0, d, LANES)
                ],
                0,
            )
        point(b, POINTS - 1)
        return carry

    lax.fori_loop(0, 2 * blocks, block, 0)
    serve_all(finish, total, units)

    def sent(q, carry):
        @pl.when(jnp.logical_and(valid(q), jnp.logical_not(valid(q + SLOTS))))
        def _():
            each(q, lambda c: c.wait_send())

        return carry

    lax.fori_loop(0, total, sent, 0)

    def written(u, carry):
        own(u, lambda c: c.wait())
        return carry

    lax.fori_loop(0, units, written, 0)


def train(n, x, dy, wg, wu, wd):
    (tokens, d), (layers, _, ff) = x.shape, wg.shape
    full, lanes = ff // FB, 3 * FB // LANES
    units = layers * full + 1
    assert layers == 2 and 2 * d <= tokens and ff % FB == LANES and d % (16 * n) == 0 and LANES // n * (d // LANES) == d // n
    assert DOWN_ROWS <= d and -(-ff // DOWN_ROWS) <= units and d // LANES <= lanes
    assert SLOTS % (n // 2) == 0 and LEAD + 1 <= SLOTS // (n // 2)
    dma, vmem = pltpu.SemaphoreType.DMA, lambda *shape: pltpu.VMEM(shape, bf16)
    return pl.pallas_call(
        functools.partial(train_kernel, n),
        out_shape=tuple(jax.ShapeDtypeStruct((size, lanes, d // n, LANES), bf16) for size in (full + 1, full)),
        in_specs=[ANY] * 5,
        out_specs=(ANY,) * 2,
        scratch_shapes=[
            vmem(tokens, d), vmem(d, tokens), vmem(tokens, d), vmem(tokens, ff), vmem(tokens, ff),
            vmem(tokens, FB), vmem(2, d, FB), vmem(2, d, FB), vmem(2, FB, d), vmem(d, ff), vmem(d, ff),
            vmem(2, F_ROWS, d), vmem(tokens, d), vmem(units, lanes, d, LANES),
            vmem(SLOTS, lanes, d // n, LANES), vmem(SLOTS, lanes, d // n, LANES),
            dma((3, 2)), dma((3,)), dma((-(-ff // DOWN_ROWS), d // LANES)), dma((2,)), dma((2,)), dma((SLOTS,)), dma((SLOTS,)), dma((SLOTS,)), dma((SLOTS,)),
            pltpu.SemaphoreType.REGULAR((SLOTS,)), pltpu.SemaphoreType.REGULAR((SLOTS,)), dma((units,)),
        ],
        compiler_params=pltpu.CompilerParams(collective_id=0, has_side_effects=True, vmem_limit_bytes=67043328),
        cost_estimate=pl.CostEstimate(flops=30 * tokens * d * ff, bytes_accessed=40 * d * ff, transcendentals=0),
        name="train",
    )(x, dy, wg, wu, wd)


def gather(n, mine):
    right, left = [(i, (i + 1) % n) for i in range(n)], [(i, (i - 1) % n) for i in range(n)]

    def both(to_right, to_left):
        from_left = lax.ppermute(to_right, "dp", right)
        return from_left, lax.ppermute(to_left, "dp", left)

    from_left = from_right = mine
    rounds = [[(0, mine)]]
    for r in range(1, n // 2):
        from_left, from_right = both(from_left, from_right)
        rounds.append([(n - r, from_left), (r, from_right)])
    half = mine.shape[1] // 2
    return [*rounds, [(n // 2, both(from_left[:, :half], from_right[:, half:]))]]


def adamw_kernel(entries, paired, side, counts, aliased, ids_ref, *refs):
    per = 2 if paired else 1
    grads, refs = refs[: entries * per * len(counts)], refs[entries * per * len(counts) :]
    ins, outs = refs[:9], refs[9 + 9 * aliased :]
    w, m, v = ins[:3], ins[3:6], ins[6:]
    fine, steps = w[2].shape[1], w[2].shape[2] // LANES
    lanes = grads[0].shape[1] * per
    half = lanes // 2
    full = counts[0] - (len(counts) == 1)
    places = [(0, unit, h) for unit in range(full) for h in range(2)]
    places.append((len(counts) - 1, full if len(counts) == 1 else 0, side))

    def step(e):
        def part(j, carry):
            rows = pl.ds(pl.multiple_of(j * fine, fine), fine)
            tile = pl.ds(pl.multiple_of(j * LANES, LANES), LANES)

            def lane(source, unit, k):
                refs = grads[(source * entries + e) * per : (source * entries + e + 1) * per]
                return wide(refs[k // half][unit, k % half, rows] if paired else refs[0][unit, k, rows])

            for at, (source, unit, h) in enumerate(places):
                cols = slice(at * LANES, (at + 1) * LANES)
                for i, where, k in ((0, (rows, cols), h), (1, (rows, cols), half + h), (2, (at, slice(None), tile), half - 1 + half * h)):
                    new = adamw(wide(w[i][where]), m[i][where], v[i][where], lane(source, unit, k))
                    for out, value in zip(outs[i::3], new, strict=True):
                        out[where] = value
            return carry

        lax.fori_loop(0, steps, part, 0)

    for e in range(entries):
        pl.when(pl.program_id(0) == e)(functools.partial(step, e))


def optimizer(n, layer, me, shards, mixed, arrays, before):
    paired = isinstance(shards[0][1], tuple)
    flat = lambda many: [a for _, b in many for a in (b if paired else (b,))]
    grads = flat(shards) + (flat(mixed) if mixed else [])
    rows = grads[0].shape[2]
    _, d, ff = arrays[0].shape
    steps = d // LANES
    assert rows % steps == 0 and rows // steps == LANES // n
    fine = rows // steps
    ids = jnp.concatenate([lax.rem(me + o, n) for o, _ in shards])

    def block(array, whole):
        units = array.shape[0]
        if whole:
            return pl.BlockSpec(array.shape, lambda i, _: (0, 0, 0, 0), pipeline_mode=pl.Buffered(1))
        return pl.BlockSpec((1, *array.shape[1:]), lambda i, _: (units - 1, 0, 0, 0), pipeline_mode=pl.Buffered(1))

    per = 2 if paired else 1
    specs = [block(a, k < len(shards) * per) for k, a in enumerate(grads)]
    up = pl.BlockSpec((None, rows, ff), lambda i, ids: (layer, ids[i], 0))
    down = pl.BlockSpec((None, ff // LANES, fine, d), lambda i, ids: (layer, 0, ids[i], 0))
    spec = [up, up, down] * 3
    counts = [shards[0][1][0].shape[0] if paired else shards[0][1].shape[0]] + ([1] if mixed else [])
    old = () if before is None else before
    return pl.pallas_call(
        functools.partial(adamw_kernel, len(shards), paired, 1 - layer, counts, bool(old)),
        out_shape=tuple(jax.ShapeDtypeStruct(a.shape, a.dtype) for a in arrays),
        grid_spec=pltpu.PrefetchScalarGridSpec(
            num_scalar_prefetch=1, grid=(len(shards),), in_specs=specs + spec + [ANY] * len(old), out_specs=tuple(spec)
        ),
        input_output_aliases={1 + len(grads) + 9 + i: i for i in range(len(old))},
        compiler_params=pltpu.CompilerParams(vmem_limit_bytes=60 * MIB),
        cost_estimate=pl.CostEstimate(
            flops=len(shards) * rows * ff * 3 * 4000, bytes_accessed=len(shards) * rows * ff * 3 * 22, transcendentals=0
        ),
        name="adamw",
    )(ids, *grads, *arrays, *old)


def solution(mesh):
    n = mesh.shape["dp"]

    def step(x, dy, *arrays):
        wg, wu, wd = arrays[:3]
        x, dy = x[0], dy[0]
        second, first = train(n, x, dy, wg, wu, wd)
        me = lax.axis_index("dp").astype(jnp.int32)[None]
        shapes = [a.shape for a in arrays]
        arrays = [a.reshape(a.shape[0], -1, LANES, a.shape[2]) if i % 3 == 2 else a for i, a in enumerate(arrays)]
        new = None
        for of_second, of_first in zip(gather(n, second), gather(n, first), strict=True):
            new = optimizer(n, 1, me, of_second, None, arrays, new)
            new = optimizer(n, 0, me, of_first, of_second, arrays, new)
        return tuple(a.reshape(shape) for a, shape in zip(new, shapes, strict=True))

    return jax.shard_map(
        step,
        mesh=mesh,
        in_specs=(P(("rep", "dp"), None, None),) * 2 + (P(None, None, None),) * 9,
        out_specs=(P("rep", None, None),) * 9,
        check_vma=False,
    )
```

```python
import functools

import jax
import jax.numpy as jnp
from jax import lax
from jax.experimental import pallas as pl
from jax.experimental.pallas import tpu as pltpu
from jax.sharding import PartitionSpec as P


LANES = 128
FB = 2 * LANES
F_ROWS = 512
DOWN_ROWS = 512
S1_ROWS = 256
STAGGER = 2
LEAD = 2
SLOTS = 12
S1_PARTS = 1
POINTS = S1_PARTS + 1
ALONE = 4
PACE = ((15, 10), (3, 2), (4, 3))
MIB = 1 << 20
MESH = pl.DeviceIdType.MESH
ANY = pl.BlockSpec(memory_space=pl.ANY)
bf16, f32 = jnp.bfloat16, jnp.float32


def wide(x):
    return x.astype(f32)


def dot(a, b, dims=((1,), (0,))):
    return lax.dot_general(a, b, (dims, ((), ())), preferred_element_type=f32)


def normed(h):
    h = wide(h)
    return (h * lax.rsqrt(jnp.mean(h * h, -1, keepdims=True) + 1e-6)).astype(bf16)


def adamw(w, m, v, g):
    m = 0.9 * m + 0.1 * g
    v = 0.95 * v + 0.05 * g * g
    step = m * lax.rsqrt(v + 1e-8) + 0.1 * w
    return (w - 0.02 * step).astype(bf16), m, v


def train_kernel(n, *refs):
    (x, dy, wg, wu, wd, *out_refs), refs = refs[:7], refs[7:]
    (av, atv, dv, dgv, duv, actv, wgr, wur, wdr, wgf, wuf, hv, h1v, g_ref, ra, rb) = refs[:16]
    (sem_w, sem_in, sem_down, sem_full, sem_x, sem_sa, sem_ra, sem_sb, sem_rb, free_a, free_b, sem_out) = refs[16:]
    tokens, d = av.shape
    ff = wg.shape[-1]
    units, lanes = g_ref.shape[:2]
    half = lanes // 2
    full = ff // FB
    blocks = full + 1
    rows = d // n
    rounds = n // 2

    me = lax.axis_index("dp")
    right, left = lax.rem(me + 1, n), lax.rem(me + n - 1, n)

    def shard(s):
        return pl.ds(pl.multiple_of(lax.rem(s, n) * rows, 16), rows)

    total = (units + STAGGER * (rounds - 1)) * rounds

    def turn(q):
        return rounds - 1 - lax.rem(q, rounds)

    def unit(q):
        return q // rounds - STAGGER * turn(q)

    def valid(q):
        return jnp.logical_and(q >= 0, jnp.logical_and(unit(q) >= 0, unit(q) < units))

    def copies(q, both):
        u, r, s = unit(q), turn(q), lax.rem(q, SLOTS)
        ca, cb = (pl.ds(0, lanes),) * 2 if both else (pl.ds(0, half), pl.ds(half, half))
        return (
            lambda: pltpu.make_async_remote_copy(
                g_ref.at[u, ca, shard(me + rounds - r)], ra.at[s, ca], sem_sa.at[s], sem_ra.at[s],
                device_id={"dp": right}, device_id_type=MESH,
            ),
            lambda: pltpu.make_async_remote_copy(
                g_ref.at[u, cb, shard(me + n - rounds + r)], rb.at[s, cb], sem_sb.at[s], sem_rb.at[s],
                device_id={"dp": left}, device_id_type=MESH,
            ),
        )

    def each(q, what, sides=(0, 1)):
        r = turn(q)

        @pl.when(r == 0)
        def _():
            for side in sides:
                what(copies(q, False)[side]())

        @pl.when(r > 0)
        def _():
            for side in sides:
                what(copies(q, True)[side]())

    free = free_a, free_b

    def send(q, sides=(0, 1)):
        @pl.when(valid(q))
        def _():
            @pl.when(valid(q - SLOTS))
            def _():
                for side in sides:
                    pl.semaphore_wait(free[side].at[lax.rem(q, SLOTS)], 1)
                each(q - SLOTS, lambda c: c.wait_send(), sides)

            each(q, lambda c: c.start(), sides)

    def own(u, what):
        def to(out, k):
            what(pltpu.make_async_copy(g_ref.at[u, :, shard(me)], out.at[k], sem_out.at[u]))

        @pl.when(u < full)
        def _():
            to(out_refs[0], u)

        @pl.when(u == units - 1)
        def _():
            to(out_refs[0], full)

        @pl.when(jnp.logical_and(u >= full, u < units - 1))
        def _():
            to(out_refs[1], u - full)

    def start(u):
        send(u * rounds + rounds - 1)

    def serve(q, ready):
        @pl.when(valid(q))
        def _():
            u, r, s = unit(q), turn(q), lax.rem(q, SLOTS)
            at, bt = shard(me + rounds - 1 - r), shard(me + n - rounds + 1 + r)

            def done_with(side):
                @pl.when(valid(q + SLOTS))
                def _():
                    to = (left, right)[side]
                    pl.semaphore_signal(free[side].at[s], inc=1, device_id={"dp": to}, device_id_type=MESH)

            for side, (got, where, lo, hi) in enumerate(((ra, at, 0, half), (rb, bt, half, lanes))):
                each(q, lambda c: c.wait_recv(), (side,))

                @pl.when(r == 0)
                def _(got=got, where=where, lo=lo, hi=hi):
                    g_ref[u, lo:hi, where] = (wide(g_ref[u, lo:hi, where]) + wide(got[s, lo:hi])).astype(bf16)

                @pl.when(jnp.logical_and(r > 0, r < rounds - 1))
                def _(got=got, where=where):
                    g_ref[u, :, where] = (wide(g_ref[u, :, where]) + wide(got[s])).astype(bf16)

                @pl.when(r < rounds - 1)
                def _(side=side):
                    send(q + STAGGER * rounds - 1, (side,))
                    done_with(side)

            @pl.when(r == rounds - 1)
            def _():
                g_ref[u, :, at] = (wide(g_ref[u, :, at]) + wide(ra[s]) + wide(rb[s])).astype(bf16)
                done_with(0)
                done_with(1)

            @pl.when(r == rounds - 1)
            def _():
                own(u, lambda c: c.start())

            @pl.when(jnp.logical_and(r == 0, u + LEAD < ready))
            def _():
                start(u + LEAD)

    def serve_all(first, last, ready):
        def one(q, carry):
            serve(q, ready)
            return carry

        lax.fori_loop(first, last, one, 0)

    def paced(pace, k):
        return k * pace[0] // pace[1]

    first = (ALONE - 1) * rounds + paced(PACE[0], POINTS * (blocks - ALONE))
    later = first + paced(PACE[1], tokens // F_ROWS)
    finish = later + paced(PACE[2], POINTS * blocks)

    def served(b, i):
        regular = jnp.where(
            b < blocks,
            (ALONE - 1) * rounds + paced(PACE[0], POINTS * (b - ALONE) + i + 1),
            later + paced(PACE[2], POINTS * (b - blocks) + i + 1),
        )
        alone = jnp.maximum(b - 1 + (i == POINTS - 1), 0) * rounds
        return jnp.where(b < ALONE, alone, regular)

    def ready(b):
        return jnp.where(b < blocks, jnp.minimum(b, full), b - 1)

    def point(b, i):
        if i < POINTS - 1:
            serve_all(served(b, i - 1), served(b, i), ready(b))
            return
        made = ready(b + 1)
        u = made - 1

        @pl.when(jnp.logical_and(made > ready(b), jnp.logical_or(u < LEAD, served(b, i - 1) >= (u - LEAD + 1) * rounds)))
        def _():
            start(u)

        serve_all(served(b, i - 1), served(b, i), made)

    loads = [
        pltpu.make_async_copy(src, dst, sem_in.at[i])
        for i, (src, dst) in enumerate(((wg.at[0], dgv.at[pl.ds(0, d)]), (wu.at[0], dgv.at[pl.ds(d, d)]), (dy, dv)))
    ]
    runs = [(i, f, min(DOWN_ROWS, ff - f)) for i, f in enumerate(range(0, ff, DOWN_ROWS))]
    downs = [
        pltpu.make_async_copy(
            wd.at[0, pl.ds(f, many), pl.ds(c * LANES, LANES)], g_ref.at[i, c, pl.ds(0, many)], sem_down.at[i, c]
        )
        for i, f, many in runs
        for c in range(d // LANES)
    ]
    whole = [pltpu.make_async_copy(src.at[1], dst, sem_full.at[i]) for i, (src, dst) in enumerate(((wg, wgf), (wu, wuf)))]

    def place(b):
        layer = jnp.where(b < blocks, 1, 0)
        j = jnp.where(b < blocks, b, b - blocks)
        return layer, j, pl.multiple_of(jnp.minimum(j * FB, ff - FB), LANES)

    def weights(b):
        layer, _, c = place(b)
        s = lax.rem(b, 2)
        return (
            pltpu.make_async_copy(wg.at[layer, :, pl.ds(c, FB)], wgr.at[s], sem_w.at[0, s]),
            pltpu.make_async_copy(wu.at[layer, :, pl.ds(c, FB)], wur.at[s], sem_w.at[1, s]),
            pltpu.make_async_copy(wd.at[layer, pl.ds(c, FB), :], wdr.at[s], sem_w.at[2, s]),
        )

    def x_tile(t):
        at = pl.ds(pl.multiple_of(t * F_ROWS, F_ROWS), F_ROWS)
        return pltpu.make_async_copy(x.at[at], hv.at[lax.rem(t, 2)], sem_x.at[lax.rem(t, 2)])

    def next_x(t):
        @pl.when(t + 1 < tokens // F_ROWS)
        def _():
            x_tile(t + 1).start()

        x_tile(t).wait()

    tiles = tokens // F_ROWS

    def normalize(t):
        r = pl.ds(pl.multiple_of(t * F_ROWS, F_ROWS), F_ROWS)
        a = normed(h1v[r, :])
        av[r, :] = a
        atv[:, r] = a.T

    def forward(t, carry):
        r = pl.ds(pl.multiple_of(t * F_ROWS, F_ROWS), F_ROWS)
        next_x(t)
        normalize(lax.rem(t + tiles - 1, tiles))
        h = hv[lax.rem(t, 2)]
        a = normed(h)
        for f in range(0, ff, FB):
            cols = slice(f, min(f + FB, ff))
            gate, up = dot(a, dgv[:d, cols]), dot(a, dgv[d : 2 * d, cols])
            duv[:F_ROWS, cols] = (gate * jax.nn.sigmoid(gate) * up).astype(bf16)
        down = sum(
            dot(duv[:F_ROWS, f : f + many], jnp.concatenate([g_ref[i, c, :many] for c in range(d // LANES)], 1))
            for i, f, many in runs
        )
        h = h + down.astype(bf16)
        h1v[r, :] = h
        return carry

    x_tile(jnp.int32(0)).start()
    for copy in (*loads[:2], *downs, loads[2], *weights(jnp.int32(0))):
        copy.start()
    barrier = pltpu.get_barrier_semaphore()
    for neighbour in (left, right):
        pl.semaphore_signal(barrier, inc=1, device_id={"dp": neighbour}, device_id_type=MESH)
    for copy in (*loads[:2], *downs):
        copy.wait()
    lax.fori_loop(0, tiles, forward, 0)
    normalize(tiles - 1)
    loads[2].wait()
    pl.semaphore_wait(barrier, 2)

    def through_norm():
        for copy in whole:
            copy.wait()
        x_tile(jnp.int32(0)).start()

        def tile(t, carry):
            r = pl.ds(pl.multiple_of(t * F_ROWS, F_ROWS), F_ROWS)
            next_x(t)
            a = normed(hv[lax.rem(t, 2)])
            av[r, :] = a
            atv[:, r] = a.T
            last = ((1,), (1,))
            da = wide(dot(dgv[r, :], wgf[...], last).astype(bf16)) + wide(dot(duv[r, :], wuf[...], last).astype(bf16))
            da = wide(da.astype(bf16))
            h = wide(h1v[r, :])
            scale = lax.rsqrt(jnp.mean(h * h, -1, keepdims=True) + 1e-6)
            dh = (da * scale - h * (scale * scale * scale * jnp.mean(da * h, -1, keepdims=True))).astype(bf16)
            dh = (wide(dv[r, :]) + wide(dh)).astype(bf16)
            dv[r, :] = dh
            serve_all(first + paced(PACE[1], t), first + paced(PACE[1], t + 1), full)
            return carry

        lax.fori_loop(0, tokens // F_ROWS, tile, 0)

    def block(b, carry):
        layer, j, c = place(b)
        s = lax.rem(b, 2)
        cols = pl.ds(c, FB)
        for copy in weights(b):
            copy.wait()

        @pl.when(b + 1 < 2 * blocks)
        def _():
            for copy in weights(b + 1):
                copy.start()

        @pl.when(b == 1)
        def _():
            for copy in whole:
                copy.start()

        @pl.when(b == blocks)
        def _():
            through_norm()

        def products(r):
            return dot(av[r, :], wgr[s]), dot(av[r, :], wur[s]), dot(dv[r, :], wdr[s], ((1,), (1,)))

        def pointwise(r, gate, up, dact):
            dact = wide(dact.astype(bf16))
            sig = jax.nn.sigmoid(gate)
            silu = gate * sig
            actv[r, :] = (silu * up).astype(bf16)
            duv[r, cols] = (dact * silu).astype(bf16)
            dgv[r, cols] = (dact * up * (sig + silu * (1.0 - sig))).astype(bf16)

        for i in range(S1_PARTS):
            before = None
            for t in range(tokens // S1_ROWS // S1_PARTS * i, tokens // S1_ROWS // S1_PARTS * (i + 1)):
                r = slice(t * S1_ROWS, (t + 1) * S1_ROWS)
                made = products(r)
                if before is not None:
                    pointwise(*before)
                before = (r, *made)
            pointwise(*before)
            point(b, i)

        rest = j == full
        u = jnp.where(rest, units - 1, jnp.where(layer == 1, j, full + j))
        h0, h1_ = jnp.where(rest, 1 - layer, 0), jnp.where(rest, 1 - layer, 1)
        dwg = dot(atv[...], dgv[:, cols]).astype(bf16)
        dwu = dot(atv[...], duv[:, cols]).astype(bf16)
        dwd = dot(actv[...], dv[...], ((0,), (0,))).astype(bf16)
        for h, k in ((h0, 0), (h1_, LANES)):
            g_ref[u, h] = dwg[:, k : k + LANES]
            g_ref[u, half + h] = dwu[:, k : k + LANES]
            g_ref[u, half - 1 + half * h] = jnp.concatenate(
                [
                    dwd[k + LANES // n * s_ : k + LANES // n * (s_ + 1), c_ : c_ + LANES]
                    for s_ in range(n)
                    for c_ in range(0, d, LANES)
                ],
                0,
            )
        point(b, POINTS - 1)
        return carry

    lax.fori_loop(0, 2 * blocks, block, 0)
    serve_all(finish, total, units)

    def sent(q, carry):
        @pl.when(jnp.logical_and(valid(q), jnp.logical_not(valid(q + SLOTS))))
        def _():
            each(q, lambda c: c.wait_send())

        return carry

    lax.fori_loop(0, total, sent, 0)

    def written(u, carry):
        own(u, lambda c: c.wait())
        return carry

    lax.fori_loop(0, units, written, 0)


def train(n, x, dy, wg, wu, wd):
    (tokens, d), (layers, _, ff) = x.shape, wg.shape
    full, lanes = ff // FB, 3 * FB // LANES
    units = layers * full + 1
    assert layers == 2 and 2 * d <= tokens and ff % FB == LANES and d % (16 * n) == 0 and LANES // n * (d // LANES) == d // n
    assert DOWN_ROWS <= d and -(-ff // DOWN_ROWS) <= units and d // LANES <= lanes
    assert SLOTS % (n // 2) == 0 and LEAD + 1 <= SLOTS // (n // 2)
    dma, vmem = pltpu.SemaphoreType.DMA, lambda *shape: pltpu.VMEM(shape, bf16)
    return pl.pallas_call(
        functools.partial(train_kernel, n),
        out_shape=tuple(jax.ShapeDtypeStruct((size, lanes, d // n, LANES), bf16) for size in (full + 1, full)),
        in_specs=[ANY] * 5,
        out_specs=(ANY,) * 2,
        scratch_shapes=[
            vmem(tokens, d), vmem(d, tokens), vmem(tokens, d), vmem(tokens, ff), vmem(tokens, ff),
            vmem(tokens, FB), vmem(2, d, FB), vmem(2, d, FB), vmem(2, FB, d), vmem(d, ff), vmem(d, ff),
            vmem(2, F_ROWS, d), vmem(tokens, d), vmem(units, lanes, d, LANES),
            vmem(SLOTS, lanes, d // n, LANES), vmem(SLOTS, lanes, d // n, LANES),
            dma((3, 2)), dma((3,)), dma((-(-ff // DOWN_ROWS), d // LANES)), dma((2,)), dma((2,)), dma((SLOTS,)), dma((SLOTS,)), dma((SLOTS,)), dma((SLOTS,)),
            pltpu.SemaphoreType.REGULAR((SLOTS,)), pltpu.SemaphoreType.REGULAR((SLOTS,)), dma((units,)),
        ],
        compiler_params=pltpu.CompilerParams(collective_id=0, has_side_effects=True, vmem_limit_bytes=67043328),
        cost_estimate=pl.CostEstimate(flops=30 * tokens * d * ff, bytes_accessed=40 * d * ff, transcendentals=0),
        name="train",
    )(x, dy, wg, wu, wd)


def gather(n, mine):
    right, left = [(i, (i + 1) % n) for i in range(n)], [(i, (i - 1) % n) for i in range(n)]

    def both(to_right, to_left):
        from_left = lax.ppermute(to_right, "dp", right)
        return from_left, lax.ppermute(to_left, "dp", left)

    from_left = from_right = mine
    rounds = [[(0, mine)]]
    for r in range(1, n // 2):
        from_left, from_right = both(from_left, from_right)
        rounds.append([(n - r, from_left), (r, from_right)])
    half = mine.shape[1] // 2
    return [*rounds, [(n // 2, both(from_left[:, :half], from_right[:, half:]))]]


def adamw_kernel(entries, paired, side, counts, aliased, ids_ref, *refs):
    per = 2 if paired else 1
    grads, refs = refs[: entries * per * len(counts)], refs[entries * per * len(counts) :]
    ins, outs = refs[:9], refs[9 + 9 * aliased :]
    w, m, v = ins[:3], ins[3:6], ins[6:]
    fine, steps = w[2].shape[1], w[2].shape[2] // LANES
    lanes = grads[0].shape[1] * per
    half = lanes // 2
    full = counts[0] - (len(counts) == 1)
    places = [(0, unit, h) for unit in range(full) for h in range(2)]
    places.append((len(counts) - 1, full if len(counts) == 1 else 0, side))

    def step(e):
        def part(j, carry):
            rows = pl.ds(pl.multiple_of(j * fine, fine), fine)
            tile = pl.ds(pl.multiple_of(j * LANES, LANES), LANES)

            def lane(source, unit, k):
                refs = grads[(source * entries + e) * per : (source * entries + e + 1) * per]
                return wide(refs[k // half][unit, k % half, rows] if paired else refs[0][unit, k, rows])

            for at, (source, unit, h) in enumerate(places):
                cols = slice(at * LANES, (at + 1) * LANES)
                for i, where, k in ((0, (rows, cols), h), (1, (rows, cols), half + h), (2, (at, slice(None), tile), half - 1 + half * h)):
                    new = adamw(wide(w[i][where]), m[i][where], v[i][where], lane(source, unit, k))
                    for out, value in zip(outs[i::3], new, strict=True):
                        out[where] = value
            return carry

        lax.fori_loop(0, steps, part, 0)

    for e in range(entries):
        pl.when(pl.program_id(0) == e)(functools.partial(step, e))


def optimizer(n, layer, me, shards, mixed, arrays, before):
    paired = isinstance(shards[0][1], tuple)
    flat = lambda many: [a for _, b in many for a in (b if paired else (b,))]
    grads = flat(shards) + (flat(mixed) if mixed else [])
    rows = grads[0].shape[2]
    _, d, ff = arrays[0].shape
    steps = d // LANES
    assert rows % steps == 0 and rows // steps == LANES // n
    fine = rows // steps
    ids = jnp.concatenate([lax.rem(me + o, n) for o, _ in shards])

    def block(array, whole):
        units = array.shape[0]
        if whole:
            return pl.BlockSpec(array.shape, lambda i, _: (0, 0, 0, 0), pipeline_mode=pl.Buffered(1))
        return pl.BlockSpec((1, *array.shape[1:]), lambda i, _: (units - 1, 0, 0, 0), pipeline_mode=pl.Buffered(1))

    per = 2 if paired else 1
    specs = [block(a, k < len(shards) * per) for k, a in enumerate(grads)]
    up = pl.BlockSpec((None, rows, ff), lambda i, ids: (layer, ids[i], 0))
    down = pl.BlockSpec((None, ff // LANES, fine, d), lambda i, ids: (layer, 0, ids[i], 0))
    spec = [up, up, down] * 3
    counts = [shards[0][1][0].shape[0] if paired else shards[0][1].shape[0]] + ([1] if mixed else [])
    old = () if before is None else before
    return pl.pallas_call(
        functools.partial(adamw_kernel, len(shards), paired, 1 - layer, counts, bool(old)),
        out_shape=tuple(jax.ShapeDtypeStruct(a.shape, a.dtype) for a in arrays),
        grid_spec=pltpu.PrefetchScalarGridSpec(
            num_scalar_prefetch=1, grid=(len(shards),), in_specs=specs + spec + [ANY] * len(old), out_specs=tuple(spec)
        ),
        input_output_aliases={1 + len(grads) + 9 + i: i for i in range(len(old))},
        compiler_params=pltpu.CompilerParams(vmem_limit_bytes=60 * MIB),
        cost_estimate=pl.CostEstimate(
            flops=len(shards) * rows * ff * 3 * 4000, bytes_accessed=len(shards) * rows * ff * 3 * 22, transcendentals=0
        ),
        name="adamw",
    )(ids, *grads, *arrays, *old)


def solution(mesh):
    n = mesh.shape["dp"]

    def step(x, dy, *arrays):
        wg, wu, wd = arrays[:3]
        x, dy = x[0], dy[0]
        second, first = train(n, x, dy, wg, wu, wd)
        me = lax.axis_index("dp").astype(jnp.int32)[None]
        shapes = [a.shape for a in arrays]
        arrays = [a.reshape(a.shape[0], -1, LANES, a.shape[2]) if i % 3 == 2 else a for i, a in enumerate(arrays)]
        new = None
        for of_second, of_first in zip(gather(n, second), gather(n, first), strict=True):
            new = optimizer(n, 1, me, of_second, None, arrays, new)
            new = optimizer(n, 0, me, of_first, of_second, arrays, new)
        return tuple(a.reshape(shape) for a, shape in zip(new, shapes, strict=True))

    return jax.shard_map(
        step,
        mesh=mesh,
        in_specs=(P(("rep", "dp"), None, None),) * 2 + (P(None, None, None),) * 9,
        out_specs=(P("rep", None, None),) * 9,
        check_vma=False,
    )
```
